256 devices in a mesh: group: 2 (over z_hi), ctx: 16 (over z_lo, y), exp: 8 (over x, core).
Axes of the slice: x: 4, y: 4, z: 8 (z_hi: 2, z_lo: 4; z = z_hi * 4 + z_lo), core: 2. Of those that a mesh axis runs over, the one named last changes fastest.
Arguments:
- prompt_query: bfloat16 [2, 8, 4096, 2048], P('group', 'exp', 'ctx'), may hold values from -6 to 6
- prompt_keys: bfloat16 [2, 8, 4096, 256], P('group', 'exp', 'ctx'), may hold values from -6 to 6
- prompt_values: bfloat16 [2, 8, 4096, 256], P('group', 'exp', 'ctx'), may hold values from -24 to 24
- lengths: int32 [2, 8], P(None, 'exp'), may hold values from 2049 to 4096
- decode_query: bfloat16 [2, 8, 256, 2048], P('group', 'exp', None, 'ctx'), may hold values from -6 to 6
- fresh_keys: bfloat16 [2, 8, 256, 256], P('group', 'exp'), may hold values from -6 to 6
- fresh_values: bfloat16 [2, 8, 256, 256], P('group', 'exp'), may hold values from -24 to 24
- x_dec: bfloat16 [2, 8, 256, 2048], P('group', 'exp', 'ctx'), may hold values from -0.59765625 to 0.59765625
- w_out: bfloat16 [2048, 2048], P('ctx'), may hold values from -0.125 to 0.125
- norm_gain: bfloat16 [2048], replicated, may hold values from 0.5 to 1.5
- w_gate_up: bfloat16 [128, 2048, 1536], P(('ctx', 'exp')), may hold values from -0.125 to 0.125
- w_down: bfloat16 [128, 768, 2048], P(('ctx', 'exp')), may hold values from -0.21875 to 0.21875
- expert_ids: int32 [2, 8, 256, 8], P('group', 'exp', 'ctx'), may hold values from 0 to 127, all different within a row; in each aligned block of 16 rows (0 to 15, 16 to 31, ..., all dimensions but the last counted through in order) at most 2 rows name the same one
- gate_weights: float32 [2, 8, 256, 8], P('group', 'exp', 'ctx'), may hold values from 0.1 to 1
Outputs:
- prompt_attention: bfloat16 [2, 8, 4096, 2048], P('group', 'exp', 'ctx')
- out_dec: bfloat16 [2, 8, 256, 2048], P('group', 'exp', 'ctx')
The draws below stay inside these ranges and needn't reach their ends.
Inputs may be any that keep to these rules, and one draw needn't show every extreme that they name: `expert_ids`: the 8 experts of a row differ; among the rows of one device no expert is named more than 2 times.
All inputs are finite; a program needn't handle non-finite values.
Results may differ from the reference program's by a relative error of at most 0.025.
Values may be sent and summed in bfloat16 or wider, within the bound.
No kernel may reach another device: no remote copies, remote signals or barrier semaphores. Data moves between devices by JAX's collectives and lax.ppermute only.
A program may use at most 128 MiB of HBM per device.

```python
import math
import jax
import jax.numpy as jnp
import numpy as np
from jax import lax

D = 2048
FF = 768
HEAD_SIZE = 128
QUERY_HEADS = 16
KEY_VALUE_HEADS = 2
TOP = 8
ROWS_DEV = 16
PROMPT_SLOTS = 4096
DECODE_REQUESTS = 256
EXPERTS = 128
CAP = 2
N_CTX = 16
N_EXP = 8


def bare_values(key, shape):
    return jnp.clip(jax.random.normal(key, shape, jnp.float32), -6.0, 6.0)


def draw_prompt_query(key, part):
    value_tensor = bare_values(jax.random.fold_in(key, 11), (2, N_EXP, PROMPT_SLOTS, QUERY_HEADS, HEAD_SIZE))
    return value_tensor.reshape(2, N_EXP, PROMPT_SLOTS, QUERY_HEADS * HEAD_SIZE).astype(jnp.bfloat16)


def draw_prompt_keys(key, part):
    value_tensor = bare_values(jax.random.fold_in(key, 13), (2, N_EXP, PROMPT_SLOTS, KEY_VALUE_HEADS, HEAD_SIZE))
    return value_tensor.reshape(2, N_EXP, PROMPT_SLOTS, KEY_VALUE_HEADS * HEAD_SIZE).astype(jnp.bfloat16)


def draw_decode_query(key, part):
    value_tensor = bare_values(jax.random.fold_in(key, 17), (2, N_EXP, DECODE_REQUESTS, QUERY_HEADS, HEAD_SIZE))
    return value_tensor.reshape(2, N_EXP, DECODE_REQUESTS, QUERY_HEADS * HEAD_SIZE).astype(jnp.bfloat16)


def touch_ends(drawn, stream_key, least, largest):
    shape = drawn.shape
    spot = [jax.random.randint(jax.random.fold_in(stream_key, axis), (), 0, shape[axis]) for axis in range(len(shape))]
    drawn = drawn.at[tuple(spot)].set(least)
    longest = shape.index(max(shape))
    spot[longest] = (spot[longest] + 1) % shape[longest]
    return drawn.at[tuple(spot)].set(largest)


def block_scale(key, extent, shards, low, largest):
    def one(position, shards_of):
        heights = jax.random.uniform(jax.random.fold_in(jax.random.fold_in(key, 6), position), (shards_of,), jnp.float32, low / len(shards), largest / len(shards))
        return jnp.repeat(jnp.exp(heights), extent[position] // shards_of).reshape((-1,) + (1,) * (len(extent) - position - 1))

    gain = one(*shards[0])
    for cut in shards[1:]:
        gain = gain * one(*cut)
    return gain


def assign_block(stream_key, own, number, rows, count, top, most, lean):
    order = jax.random.permutation(stream_key, count)
    heavy_load, usual = load_shares(count, rows * top, most, lean, True), load_shares(count, rows * top, most, lean, False)
    places = jnp.arange(count)

    def named(tallies, turn):
        used = int((tallies > 0).sum())
        fixed = max(1, used // 4)
        passed = fixed + (places - fixed + turn * (used - fixed)) % max(1, count - fixed)
        return jnp.zeros((count,), jnp.int32).at[order[jnp.where(places < fixed, places, passed)]].set(jnp.asarray(tallies, jnp.int32))

    tallies = jnp.where(number % 4 == 0, named(heavy_load, number // 4), named(usual, number - number // 4 - 1))
    mixed = jax.random.permutation(jax.random.fold_in(own, 3), count)
    giver, taker = mixed[0:count // 2 * 2:2], mixed[1:count // 2 * 2:2]
    slack = jnp.minimum(tallies[giver] - 1, most - tallies[taker]) // 2
    slack = jnp.where((giver == order[0]) | (taker == order[0]) | (tallies[taker] == 0), 0, jnp.maximum(slack, 0))
    passed = jax.random.randint(jax.random.fold_in(own, 4), (count // 2,), 0, 1 << 20) % (slack + 1)
    tallies = tallies.at[giver].add(-passed).at[taker].add(passed)
    labels = jnp.searchsorted(jnp.cumsum(tallies), jnp.arange(rows * top), side="right").astype(jnp.int32)
    table = labels.reshape(top, rows).T
    table = table[jax.random.permutation(jax.random.fold_in(own, 1), rows)]
    turn = jax.random.randint(jax.random.fold_in(own, 2), (rows, 1), 0, top)
    return jnp.take_along_axis(table, (jnp.arange(top)[None, :] + turn) % top, axis=1)


def load_shares(amount, total, limit, lean, full):
    loads = [(1 << 20) // math.isqrt(rank ** lean) + 1 for rank in range(1, amount + 1)]
    largest = limit if full else min(limit, max(-(-total // amount), total * loads[0] // sum(loads)))
    least = 1 if total - largest >= amount - 1 else 0
    holding, surplus = [largest] + [least] * (amount - 1), total - largest - least * (amount - 1)
    while surplus > 0:
        free = [i for i in range(1, amount) if holding[i] < largest] or [i for i in range(1, amount) if holding[i] < limit]
        mass, left = sum([loads[i] for i in free]), surplus
        for i in free:
            addition = min(limit - holding[i], max(1, left * loads[i] // mass), surplus)
            holding[i] = holding[i] + addition
            surplus = surplus - addition
    return np.array(holding)


def noise(own_key, extent, scale, bound, split=(), held_as=jnp.bfloat16):
    entries = scale * jax.random.normal(own_key, extent, jnp.float32)
    if split:
        entries = entries * block_scale(own_key, extent, split, -0.22, 0.18)
    return jnp.clip(entries, -bound, bound).astype(held_as)


def setup_inputs(seed: int = 0) -> dict:
    key_of = jax.random.split(jax.random.key(seed), 15)
    prompt_query = draw_prompt_query(jax.random.fold_in(key_of[14], 71), 0)
    prompt_keys = draw_prompt_keys(jax.random.fold_in(key_of[14], 71), 0)
    prompt_values = noise(key_of[2], (2, N_EXP, PROMPT_SLOTS, KEY_VALUE_HEADS * HEAD_SIZE), 4.0, 24.0, ((0, 2), (1, 8), (2, 16)))
    lengths = touch_ends(jax.random.randint(key_of[3], (2, N_EXP), PROMPT_SLOTS // 2 + 1, PROMPT_SLOTS + 1), jax.random.fold_in(key_of[3], 1), PROMPT_SLOTS // 2 + 1, PROMPT_SLOTS).astype(jnp.int32)
    decode_query = draw_decode_query(jax.random.fold_in(key_of[14], 71), 0)
    fresh_keys = noise(key_of[5], (2, N_EXP, DECODE_REQUESTS, KEY_VALUE_HEADS * HEAD_SIZE), 1.0, 6.0, ((0, 2), (1, 8)))
    fresh_values = noise(key_of[6], (2, N_EXP, DECODE_REQUESTS, KEY_VALUE_HEADS * HEAD_SIZE), 4.0, 24.0, ((0, 2), (1, 8)))
    x_dec = noise(key_of[7], (2, N_EXP, DECODE_REQUESTS, D), 0.1, 0.59765625, ((0, 2), (1, 8), (2, 16)))
    w_out = noise(key_of[8], (QUERY_HEADS * HEAD_SIZE, D), (QUERY_HEADS * HEAD_SIZE) ** -0.5, 0.125, ((0, 16),))
    norm_gain = jnp.clip(1.0 + 0.1 * jax.random.normal(key_of[9], (D,), jnp.float32), 0.5, 1.5).astype(jnp.bfloat16)
    w_gate_up = noise(key_of[10], (EXPERTS, D, 2 * FF), D ** -0.5, 0.125, ((0, 128),))
    w_down = noise(key_of[11], (EXPERTS, FF, D), FF ** -0.5, 0.21875, ((0, 128),))
    expert_ids_keys = jax.random.split(jax.random.fold_in(key_of[12], 1), 2 * N_EXP * DECODE_REQUESTS // ROWS_DEV)
    expert_ids_turns = jax.random.permutation(jax.random.fold_in(key_of[12], 3), 2 * N_EXP * DECODE_REQUESTS // ROWS_DEV)
    expert_ids = jax.vmap(lambda own, number: assign_block(jax.random.fold_in(key_of[12], 2), own, number, ROWS_DEV, EXPERTS, TOP, CAP, 1))(expert_ids_keys, expert_ids_turns).reshape((2, N_EXP, DECODE_REQUESTS, TOP))
    gate_weights = jnp.clip(jnp.exp(math.log(1.0) - 2.3025851 * jax.random.uniform(key_of[13], (2, N_EXP, DECODE_REQUESTS, TOP), jnp.float32) ** block_scale(key_of[13], (2, N_EXP, DECODE_REQUESTS, TOP), ((0, 2), (1, 8), (2, 16)), -0.2, 0.2)), 0.1, 1.0)
    return {"prompt_query": prompt_query, "prompt_keys": prompt_keys, "prompt_values": prompt_values, "lengths": lengths, "decode_query": decode_query, "fresh_keys": fresh_keys, "fresh_values": fresh_values, "x_dec": x_dec, "w_out": w_out, "norm_gain": norm_gain, "w_gate_up": w_gate_up, "w_down": w_down, "expert_ids": expert_ids, "gate_weights": gate_weights}


NEGATIVE_LIMIT = -1e+30
EPSILON = 1e-06

def reference(prompt_query, prompt_keys, prompt_values, lengths, decode_query, fresh_keys, fresh_values, x_dec, w_out, norm_gain, w_gate_up, w_down, expert_ids, gate_weights):
    group_width = QUERY_HEADS // KEY_VALUE_HEADS
    scaling = HEAD_SIZE ** (-0.5)
    block_size = math.gcd(PROMPT_SLOTS, 512)
    prompt_list = 2 * N_EXP

    def prefill_one_prompt(operands):
        query_vector, key_tensor, value_tensor, length = operands
        query_vector = query_vector.astype(jnp.float32).reshape(PROMPT_SLOTS, KEY_VALUE_HEADS, group_width, HEAD_SIZE)
        key_tensor = key_tensor.astype(jnp.float32).reshape(PROMPT_SLOTS, KEY_VALUE_HEADS, HEAD_SIZE)
        value_tensor = value_tensor.astype(jnp.float32).reshape(PROMPT_SLOTS, KEY_VALUE_HEADS, HEAD_SIZE)
        columns = jnp.arange(PROMPT_SLOTS, dtype=jnp.int32)

        def one_block(offset):
            rows_query = lax.dynamic_slice_in_dim(query_vector, offset, block_size, 0)
            row_pos = offset + jnp.arange(block_size, dtype=jnp.int32)
            scores = jnp.einsum('qhgd,khd->hgqk', rows_query, key_tensor) * scaling
            keep_mask = (columns[None, :] <= row_pos[:, None]) & (columns[None, :] < length)
            scores = jnp.where(keep_mask, scores, NEGATIVE_LIMIT)
            peak = scores.max(-1, keepdims=True)
            weights = jnp.where(keep_mask, jnp.exp(scores - peak), 0.0)
            totals = jnp.transpose(weights.sum(-1), (2, 0, 1))
            rounded = weights.astype(jnp.bfloat16).astype(jnp.float32)
            mixed = jnp.einsum('hgqk,khd->qhgd', rounded, value_tensor)
            mixed = mixed / jnp.where(totals > 0, totals, 1.0)[..., None]
            mixed = jnp.where((row_pos < length)[:, None, None, None], mixed, 0.0)
            return mixed.reshape(block_size, QUERY_HEADS * HEAD_SIZE).astype(jnp.bfloat16)
        offsets = jnp.arange(PROMPT_SLOTS // block_size, dtype=jnp.int32) * block_size
        return lax.map(one_block, offsets).reshape(PROMPT_SLOTS, QUERY_HEADS * HEAD_SIZE)
    prompt_attention = lax.map(prefill_one_prompt, (prompt_query.reshape(prompt_list, PROMPT_SLOTS, QUERY_HEADS * HEAD_SIZE), prompt_keys.reshape(prompt_list, PROMPT_SLOTS, KEY_VALUE_HEADS * HEAD_SIZE), prompt_values.reshape(prompt_list, PROMPT_SLOTS, KEY_VALUE_HEADS * HEAD_SIZE), lengths.reshape(prompt_list))).reshape(2, N_EXP, PROMPT_SLOTS, QUERY_HEADS * HEAD_SIZE)

    def decode_for_prompt(operands):
        query_vector, key_tensor, value_tensor, length, appended_keys, appended_values = operands
        query_vector = query_vector.astype(jnp.float32).reshape(DECODE_REQUESTS, KEY_VALUE_HEADS, group_width, HEAD_SIZE)
        key_tensor = key_tensor.astype(jnp.float32).reshape(PROMPT_SLOTS, KEY_VALUE_HEADS, HEAD_SIZE)
        value_tensor = value_tensor.astype(jnp.float32).reshape(PROMPT_SLOTS, KEY_VALUE_HEADS, HEAD_SIZE)
        appended_keys = appended_keys.astype(jnp.float32).reshape(DECODE_REQUESTS, KEY_VALUE_HEADS, HEAD_SIZE)
        appended_values = appended_values.astype(jnp.float32).reshape(DECODE_REQUESTS, KEY_VALUE_HEADS, HEAD_SIZE)
        columns = jnp.arange(PROMPT_SLOTS, dtype=jnp.int32)
        keep_mask = columns < length
        scores = jnp.einsum('shgd,khd->hgsk', query_vector, key_tensor) * scaling
        scores = jnp.where(keep_mask, scores, NEGATIVE_LIMIT)
        own_score = jnp.einsum('shgd,shd->hgs', query_vector, appended_keys) * scaling
        peak = jnp.maximum(scores.max(-1), own_score)
        weights = jnp.where(keep_mask, jnp.exp(scores - peak[..., None]), 0.0)
        own_weight = jnp.exp(own_score - peak)
        totals = weights.sum(-1) + own_weight
        mixed = jnp.einsum('hgsk,khd->hgsd', weights.astype(jnp.bfloat16).astype(jnp.float32), value_tensor)
        mixed = mixed + own_weight.astype(jnp.bfloat16).astype(jnp.float32)[..., None] * jnp.transpose(appended_values, (1, 0, 2))[:, None]
        mixed = mixed / totals[..., None]
        return jnp.transpose(mixed, (2, 0, 1, 3)).reshape(DECODE_REQUESTS, QUERY_HEADS * HEAD_SIZE).astype(jnp.bfloat16)
    decode_attention = lax.map(decode_for_prompt, (decode_query.reshape(prompt_list, DECODE_REQUESTS, QUERY_HEADS * HEAD_SIZE), prompt_keys[::-1].reshape(prompt_list, PROMPT_SLOTS, KEY_VALUE_HEADS * HEAD_SIZE), prompt_values[::-1].reshape(prompt_list, PROMPT_SLOTS, KEY_VALUE_HEADS * HEAD_SIZE), lengths[::-1].reshape(prompt_list), fresh_keys.reshape(prompt_list, DECODE_REQUESTS, KEY_VALUE_HEADS * HEAD_SIZE), fresh_values.reshape(prompt_list, DECODE_REQUESTS, KEY_VALUE_HEADS * HEAD_SIZE)))
    projected = jnp.dot(decode_attention.reshape(-1, QUERY_HEADS * HEAD_SIZE), w_out, preferred_element_type=jnp.float32).reshape(2, N_EXP, DECODE_REQUESTS, D)
    residual = x_dec.astype(jnp.float32) + projected
    normed = (residual * lax.rsqrt(lax.optimization_barrier(jnp.mean(residual * residual, -1, keepdims=True)) + EPSILON) * norm_gain.astype(jnp.float32)).astype(jnp.bfloat16)
    most_rows = N_CTX * N_EXP * CAP
    moe_parts = []
    for group_index in range(2):
        rows_flat = normed[group_index].reshape(-1, D)
        flat_ids = expert_ids[group_index].reshape(-1)
        flat_gates = gate_weights[group_index].reshape(-1)

        def expert_pass(carried, operands, rows_flat=rows_flat, flat_ids=flat_ids, flat_gates=flat_gates):
            gate_up, down, expert = operands
            chosen = flat_ids == expert
            slots = jnp.nonzero(chosen, size=most_rows, fill_value=0)[0].astype(jnp.int32)
            usable = jnp.arange(most_rows, dtype=jnp.int32) < jnp.sum(chosen.astype(jnp.int32))
            owners = slots // TOP
            gathered = rows_flat[owners]
            mixed = jnp.dot(gathered, gate_up, preferred_element_type=jnp.float32)
            hidden = (jax.nn.silu(mixed[:, :FF]) * mixed[:, FF:]).astype(jnp.bfloat16)
            output = jnp.dot(hidden, down, preferred_element_type=jnp.float32).astype(jnp.bfloat16).astype(jnp.float32)
            scaled = output * jnp.where(usable, flat_gates[slots], 0.0)[:, None]
            return (carried.at[owners].add(scaled), None)
        initial = jnp.zeros((N_EXP * DECODE_REQUESTS, D), jnp.float32)
        summed, unused_out = lax.scan(expert_pass, initial, (w_gate_up, w_down, jnp.arange(EXPERTS, dtype=jnp.int32)))
        moe_parts.append(summed)
    moe = jnp.stack(moe_parts).reshape(2, N_EXP, DECODE_REQUESTS, D)
    out_dec = (residual + moe).astype(jnp.bfloat16)
    return (prompt_attention, out_dec)
```

```python
import functools

import jax
import jax.numpy as jnp
from jax import lax
from jax.experimental import pallas as pl
from jax.experimental.pallas import tpu as pltpu
from jax.sharding import Mesh
from jax.sharding import PartitionSpec as P

HEAD = 128
HEADS = 16
KV = 2
BLK = 256
FAR = 1024
ROWS = 16
D = 2048
NZ = 4
NY = 4
NE = 8
NEG = -1e30
EPSILON = 1e-06
BF = jnp.bfloat16
F32 = jnp.float32
SCALE2 = float(HEAD ** (-0.5) * 1.4426950408889634)


def dot_t(a, b):
    return lax.dot_general(a, b, (((1,), (1,)), ((), ())), preferred_element_type=F32)


def dot_n(a, b):
    return lax.dot_general(a, b, (((1,), (0,)), ((), ())), preferred_element_type=F32)


def decode_kernel(sc, q_ref, k_ref, v_ref, ek_ref, ev_ref, acc_ref, st_ref):
    z, y, length = sc[0], sc[1], sc[2]
    col = lax.broadcasted_iota(jnp.int32, (1, NY * BLK), 1)
    blk_y = (y - col // BLK + NY) % NY
    pos = z * (NY * BLK) + blk_y * BLK + col % BLK
    valid = pos < length
    rows = 128
    n = q_ref.shape[0] // rows
    ocol = lax.broadcasted_iota(jnp.int32, (rows, 128), 1)
    orow = lax.broadcasted_iota(jnp.int32, (rows, 128), 0)
    own = (ocol < ROWS) & (orow % (NZ * ROWS) == z * ROWS + ocol)
    lane = lax.broadcasted_iota(jnp.int32, (rows, 128), 1)
    for i in range(n):
        q = q_ref[i * rows : (i + 1) * rows]
        s = dot_t(q, k_ref[...]) * SCALE2
        s = jnp.where(valid, s, NEG)
        so = dot_t(q, ek_ref[...]) * SCALE2
        so = jnp.where(own, so, NEG)
        m = jnp.maximum(s.max(-1, keepdims=True), so.max(-1, keepdims=True))
        m = jnp.maximum(jnp.ceil(m * 0.25) * 4.0, -1e29)
        p = jnp.exp2(s - m)
        po = jnp.exp2(so - m)
        total = p.sum(-1, keepdims=True) + po.sum(-1, keepdims=True)
        acc = dot_n(p.astype(BF), v_ref[...]) + dot_n(po.astype(BF), ev_ref[...])
        acc_ref[i * rows : (i + 1) * rows] = acc.astype(BF)
        hi = total.astype(BF).astype(F32)
        lo = total - hi
        st = jnp.where(lane == 0, m, jnp.where(lane == 1, hi, jnp.where(lane == 2, lo, 0.0)))
        st_ref[:, i * rows : (i + 1) * rows] = st.T[:8]


def decode_partial(sc, q, keys, ek, ev):
    half = q.shape[0] // KV
    return pl.pallas_call(
        decode_kernel,
        name="decode_partial",
        grid_spec=pltpu.PrefetchScalarGridSpec(
            num_scalar_prefetch=1,
            grid=(KV,),
            in_specs=[
                pl.BlockSpec((half, HEAD), lambda h, s: (h, 0)),
                pl.BlockSpec((NY * BLK, HEAD), lambda h, s: (0, h)),
                pl.BlockSpec((NY * BLK, HEAD), lambda h, s: (0, KV + h)),
                pl.BlockSpec((128, HEAD), lambda h, s: (0, h)),
                pl.BlockSpec((128, HEAD), lambda h, s: (0, h)),
            ],
            out_specs=[
                pl.BlockSpec((half, HEAD), lambda h, s: (h, 0)),
                pl.BlockSpec((8, half), lambda h, s: (0, h)),
            ],
        ),
        out_shape=[
            jax.ShapeDtypeStruct(q.shape, BF),
            jax.ShapeDtypeStruct((8, q.shape[0]), F32),
        ],
        cost_estimate=pl.CostEstimate(
            flops=4 * q.shape[0] * 1024 * 128 * 2, bytes_accessed=1 << 21, transcendentals=1 << 20
        ),
        compiler_params=pltpu.CompilerParams(vmem_limit_bytes=24 << 20),
    )(sc, q, keys, keys, ek, ev)


def prefill_kernel(sc, q_ref, k0_ref, v0_ref, kz_ref, vz_ref, *rest, heads):
    out_ref, m_ref, l_ref, acc_ref = rest[-4:]
    z, y, length = sc[0], sc[1], sc[2]
    start = (z * NY + y) * BLK

    def block(k, v, mask, first):
        for h in range(heads):
            q = q_ref[:, h * HEAD : (h + 1) * HEAD]
            s = dot_t(q, k) * SCALE2
            if mask is not None:
                s = jnp.where(mask, s, NEG)
            top = s.max(-1, keepdims=True)
            if first:
                m = jnp.broadcast_to(top, (BLK, HEAD))
            else:
                old = m_ref[h]
                m = jnp.maximum(old, top)
            n = k.shape[0] // HEAD
            p = jnp.exp2(s - jnp.concatenate([m] * n, axis=1))
            part = p[:, :HEAD]
            for c in range(1, n):
                part = part + p[:, c * HEAD : (c + 1) * HEAD]
            o = dot_n(p.astype(BF), v)
            if first:
                l_ref[h] = part
                acc_ref[h] = o
            else:
                alpha = jnp.exp2(old - m)
                l_ref[h] = l_ref[h] * alpha + part
                acc_ref[h] = acc_ref[h] * alpha + o
            m_ref[h] = m

    @pl.when(start < length)
    def _():
        row = lax.broadcasted_iota(jnp.int32, (BLK, BLK), 0)
        col = lax.broadcasted_iota(jnp.int32, (BLK, BLK), 1)
        block(k0_ref[:BLK], v0_ref[:BLK], col <= row, True)

        def near(i, c):
            at = pl.multiple_of(i * BLK, BLK)
            block(k0_ref[pl.ds(at, BLK)], v0_ref[pl.ds(at, BLK)], None, False)
            return c

        lax.fori_loop(1, y + 1, near, 0)

        def far(i, c):
            at = pl.multiple_of(i * FAR, FAR)
            block(kz_ref[pl.ds(at, FAR)], vz_ref[pl.ds(at, FAR)], None, False)
            return c

        lax.fori_loop(0, z * (NY * BLK // FAR), far, 0)
        pos = start + lax.broadcasted_iota(jnp.int32, (BLK, HEAD), 0)
        for h in range(heads):
            total = l_ref[h].sum(-1, keepdims=True)
            o = acc_ref[h] / total
            out_ref[:, h * HEAD : (h + 1) * HEAD] = jnp.where(pos < length, o, 0.0).astype(BF)

    @pl.when(start >= length)
    def _():
        out_ref[...] = jnp.zeros(out_ref.shape, BF)


def prefill_part(sc, q, near, far, part, parts, out):
    heads = HEADS // parts
    kv = part * KV // parts
    width = heads * HEAD
    in_specs = [
        pl.BlockSpec((BLK, width), lambda i, s: (0, part)),
        pl.BlockSpec((NY * BLK, HEAD), lambda i, s: (0, kv)),
        pl.BlockSpec((NY * BLK, HEAD), lambda i, s: (0, KV + kv)),
        pl.BlockSpec((3 * NY * BLK, HEAD), lambda i, s: (0, kv)),
        pl.BlockSpec((3 * NY * BLK, HEAD), lambda i, s: (0, KV + kv)),
    ]
    operands = [sc, q, near, near, far, far]
    aliases = {}
    if out is not None:
        in_specs.append(pl.BlockSpec(memory_space=pl.ANY))
        operands.append(out)
        aliases = {6: 0}
    return pl.pallas_call(
        functools.partial(prefill_kernel, heads=heads),
        name=f"prefill_{part}",
        grid_spec=pltpu.PrefetchScalarGridSpec(
            num_scalar_prefetch=1,
            grid=(1,),
            in_specs=in_specs,
            out_specs=pl.BlockSpec((BLK, width), lambda i, s: (0, part)),
            scratch_shapes=[pltpu.VMEM((heads, BLK, HEAD), F32)] * 3,
        ),
        out_shape=jax.ShapeDtypeStruct((BLK, HEADS * HEAD), BF),
        input_output_aliases=aliases,
        cost_estimate=pl.CostEstimate(
            flops=4 * heads * BLK * 4096 * HEAD * 2, bytes_accessed=3 << 20, transcendentals=heads * BLK * 4096
        ),
        compiler_params=pltpu.CompilerParams(vmem_limit_bytes=24 << 20),
    )(*operands)


def prefill(sc, q, near, far, parts=4):
    out = None
    for part in range(parts):
        out = prefill_part(sc, q, near, far, part, parts, out)
    return out


SWAP = [(0, 1), (1, 0)]


def along_y(x):
    up = [(i, (i + 1) % NY) for i in range(NY)]
    down = [(i, (i - 1) % NY) for i in range(NY)]
    half = x.shape[0] // 2
    below = lax.ppermute(x, "y", up)
    above = lax.ppermute(x, "y", down)
    opp_a = lax.ppermute(below[:half], "y", up)
    opp_b = lax.ppermute(above[half:], "y", down)
    return x, below, jnp.concatenate([opp_a, opp_b], axis=0), above


def swap_z(x):
    return lax.all_to_all(x, "z", split_axis=0, concat_axis=0, tiled=True)


def body(
    prompt_query,
    prompt_keys,
    prompt_values,
    lengths,
    decode_query,
    fresh_keys,
    fresh_values,
    x_dec,
    w_out,
    norm_gain,
    w_gate_up,
    w_down,
    expert_ids,
    gate_weights,
):
    group = lax.axis_index("group")
    z = lax.axis_index("z")
    y = lax.axis_index("y")
    ctx = z * NY + y
    length = lax.dynamic_index_in_dim(lengths[:, 0], group, keepdims=False)
    sc = jnp.stack([z, y, length]).astype(jnp.int32)

    query = lax.ppermute(decode_query[0, 0], "group", SWAP)
    fresh_k = lax.dynamic_slice_in_dim(fresh_keys[0, 0], ctx * ROWS, ROWS, 0)
    fresh_v = lax.dynamic_slice_in_dim(fresh_values[0, 0], ctx * ROWS, ROWS, 0)
    gates = gate_weights[0, 0]
    gate_hi = gates.astype(BF)
    gate_mid = (gates - gate_hi.astype(F32)).astype(BF)
    gate_lo = (gates - gate_hi.astype(F32) - gate_mid.astype(F32)).astype(BF)
    top = gates.shape[1]
    pad = jnp.zeros((ROWS, 128 - 4 * top), BF)
    misc = [expert_ids[0, 0].astype(BF), gate_hi, gate_mid, gate_lo, pad]
    packed = jnp.concatenate([x_dec[0, 0], fresh_k, fresh_v] + misc, axis=1)
    packed = lax.ppermute(packed, "group", SWAP)
    x_in = packed[:, :D]
    fresh_k = packed[:, D : D + 256]
    fresh_v = packed[:, D + 256 : D + 512]
    misc = packed[:, D + 512 :]

    keys = jnp.concatenate([prompt_keys[0, 0], prompt_values[0, 0]], axis=1)
    near = jnp.concatenate(along_y(keys), axis=0)

    split = query.reshape(NZ, NY, ROWS, HEAD).transpose(1, 0, 2, 3).reshape(NY, NZ * ROWS, HEAD)
    split = jnp.concatenate([split, jnp.broadcast_to(misc[None], (NY, ROWS, 128))], axis=1)
    rows_q = NZ * ROWS + ROWS
    send = jnp.broadcast_to(split[None], (NZ, NY, rows_q, HEAD)).reshape(NZ * NY, rows_q, HEAD)
    got = lax.all_to_all(send, ("z", "y"), split_axis=0, concat_axis=0, tiled=True)
    q_all = got[:, : NZ * ROWS].reshape(HEADS * NZ * ROWS, HEAD)
    misc_all = lax.dynamic_index_in_dim(
        got[:, NZ * ROWS :].reshape(NZ, NY, ROWS, 128), y, axis=1, keepdims=False
    )

    w_own, w_below, w_opp, w_above = along_y(w_out)
    w_near = jnp.concatenate([w_own, w_below, w_opp, w_above], axis=0)

    wide = ((0, 128 - ROWS), (0, 0))
    acc, stat = decode_partial(sc, q_all, near, jnp.pad(fresh_k, wide), jnp.pad(fresh_v, wide))
    per = HEADS * NZ * ROWS // NZ
    stat = stat.astype(BF).reshape(8, NZ, per // 128, 128).transpose(1, 0, 2, 3).reshape(NZ, 16, 128)
    parts = swap_z(jnp.concatenate([acc.reshape(NZ, per, HEAD), stat], axis=1))
    stat = parts[:, per:].reshape(NZ, 8, per).astype(F32)
    peak = stat[:, 0]
    share = jnp.exp2(peak - peak.max(0, keepdims=True))
    total = (share * (stat[:, 1] + stat[:, 2])).sum(0)
    attn = ((share / total)[..., None] * parts[:, :per].astype(F32)).sum(0)
    attn = attn.astype(BF).reshape(NZ, NZ * ROWS, HEAD)
    flipped = jnp.concatenate([attn[::-1], attn[::-1]], axis=0)
    attn = lax.dynamic_slice_in_dim(flipped, NY - 1 - y, NY, 0)
    attn = attn.transpose(1, 0, 2).reshape(NZ * ROWS, NY * HEAD)
    projected = dot_n(attn, w_near).astype(BF).reshape(NZ, ROWS, D)
    projected = swap_z(projected).astype(F32).sum(0)
    residual = x_in.astype(F32) + projected
    normed = (
        residual
        * lax.rsqrt(jnp.mean(residual * residual, -1, keepdims=True) + EPSILON)
        * norm_gain.astype(F32)
    ).astype(BF)

    local = NY * NE
    ids = misc_all[..., :top].astype(jnp.int32) - z * local
    g3 = misc_all[..., top : 4 * top].astype(F32)
    gate_all = g3[..., :top] + g3[..., top : 2 * top] + g3[..., 2 * top :]
    hit = ids[..., None] == lax.iota(jnp.int32, local)
    named = hit.any(2)
    gate_of = jnp.where(hit, gate_all[..., None], 0.0).sum(2)
    rank = jnp.cumsum(named.astype(jnp.int32), axis=1) - named.astype(jnp.int32)
    placed = named[:, None] & (rank[:, None] == lax.iota(jnp.int32, 2)[None, :, None, None])
    same = lax.iota(jnp.int32, NZ)[:, None] == lax.iota(jnp.int32, NZ)[None, :]
    spread = placed.transpose(3, 0, 1, 2)[:, :, :, None, :] & same[None, :, None, :, None]
    slots = local * NZ * 2
    place = spread.astype(BF).reshape(slots, NZ * ROWS)
    weigh = jnp.where(spread, gate_of.transpose(2, 0, 1)[:, None, None], 0.0).reshape(slots, NZ * ROWS)
    weigh_hi = weigh.astype(BF)
    weigh_lo = (weigh - weigh_hi.astype(F32)).astype(BF)

    everyone = swap_z(jnp.broadcast_to(normed[None], (NZ, ROWS, D))).reshape(NZ * ROWS, D)
    buffer = dot_n(place, everyone).astype(BF).reshape(local, NZ * 2, D)
    arrived = lax.all_to_all(buffer, ("y", "exp"), split_axis=0, concat_axis=0, tiled=True)
    mixed = dot_n(arrived.reshape(slots, D), w_gate_up[0])
    units = mixed.shape[1] // 2
    hidden = (jax.nn.silu(mixed[:, :units]) * mixed[:, units:]).astype(BF)
    produced = dot_n(hidden, w_down[0]).astype(BF).reshape(local, NZ * 2, D)
    returned = lax.all_to_all(produced, ("y", "exp"), split_axis=0, concat_axis=0, tiled=True)
    returned = returned.reshape(slots, D)
    over = (((0,), (0,)), ((), ()))
    moe = lax.dot_general(weigh_hi, returned, over, preferred_element_type=F32)
    moe = moe + lax.dot_general(weigh_lo, returned, over, preferred_element_type=F32)
    moe = swap_z(moe.astype(BF).reshape(NZ, ROWS, D)).astype(F32).sum(0)
    out_dec = lax.ppermute((residual + moe).astype(BF), "group", SWAP)

    ups = [[(i, i + s) for i in range(NZ - s)] for s in (1, 2, 3)]
    lower = jnp.concatenate([lax.ppermute(keys, "z", up) for up in ups], axis=0)
    far = jnp.stack([b.reshape(3, BLK, 512) for b in along_y(lower)], axis=1).reshape(3 * NY * BLK, 512)
    prompt_attention = prefill(sc, prompt_query[0, 0], near, far)
    return prompt_attention[None, None], out_dec[None, None]


def solution(mesh):
    mesh = Mesh(mesh.devices.reshape(2, NZ, NY, NE), ("group", "z", "y", "exp"))
    ctx = ("z", "y")
    in_specs = (
        P("group", "exp", ctx, None),
        P("group", "exp", ctx, None),
        P("group", "exp", ctx, None),
        P(None, "exp"),
        P("group", "exp", None, ctx),
        P("group", "exp", None, None),
        P("group", "exp", None, None),
        P("group", "exp", ctx, None),
        P(ctx, None),
        P(),
        P(("z", "y", "exp"), None, None),
        P(("z", "y", "exp"), None, None),
        P("group", "exp", ctx, None),
        P("group", "exp", ctx, None),
    )
    out_specs = (P("group", "exp", ctx, None), P("group", "exp", ctx, None))
    return jax.shard_map(body, mesh=mesh, in_specs=in_specs, out_specs=out_specs, check_vma=False)
```
